128 devices in a mesh: expert: 8 (over z, core), fsdp: 16 (over y, x).
Axes of the slice: x: 4, y: 4, z: 4, core: 2. Of those that a mesh axis runs over, the one named last changes fastest.
Arguments:
- hidden: bfloat16 [8, 768, 8192], P('expert', None, 'fsdp'), may hold values from -0.198873782 to 0.198873782
- expert_ids: int32 [2048, 2], P(('expert', 'fsdp')), may hold values from 0 to 7, all different within a row; in each aligned block of 16 rows (0 to 15, 16 to 31, ...) at most 6 rows name the same one
- gate_weights: float32 [2048, 2], P(('expert', 'fsdp')), may hold values from 0.2 to 1
- loss_weight: float32 [2048], P(('expert', 'fsdp')), may hold values from 0.3 to 3
- decay: float32 [1], replicated, may hold values from 0.2 to 0.6
- val_grad: bfloat16 [8, 8192, 4096], P('expert', 'fsdp'), may hold values from -8 to 8
- down_weight: bfloat16 [8, 8192, 4096], P('expert', 'fsdp'), may hold values from -0.0625 to 0.0625
Outputs:
- solution: float32 [8, 8192, 4096], P('expert', 'fsdp')
- hyper: float32 [1], replicated
The draws below stay inside these ranges and needn't reach their ends.
Inputs may be any that keep to these rules, and one draw needn't show every extreme that they name: `expert_ids`: each token names 2 different experts; among the 16 tokens of one device no expert is named more than 6 times, a bound that some block reaches.
All inputs are finite; a program needn't handle non-finite values.
Results may differ from the reference program's by a relative error of at most 0.00067.
Values may be sent and summed in bfloat16 or wider, within the bound.
No kernel may reach another device: no remote copies, remote signals or barrier semaphores. Data moves between devices by JAX's collectives and lax.ppermute only.
A program may use at most 128 MiB of HBM per device.

```python
import math
import jax
import jax.numpy as jnp
import numpy as np
from jax import lax

D = 4096
FFW = 8192
TOP = 2
ITERS = 2
TOK_DEV = 16
EXPERTS = 8
CAP = 6
TOKENS = 2048
ROWS = 768
N_EXPERT = 8
N_FSDP = 16


def unit_scales(key):
    logs = jax.random.uniform(jax.random.fold_in(key, 7301), (EXPERTS, FFW), jnp.float32, math.log(0.3), math.log(3.0))
    activity = jnp.exp(logs)
    normed = activity / jnp.sqrt(jnp.mean(activity * activity, axis=1, keepdims=True))
    return jnp.clip(normed, 0.0, 3.5)


def hidden_values(key):
    scales = unit_scales(key)
    noise = jax.random.truncated_normal(jax.random.fold_in(key, 7302), -2.5, 2.5, (EXPERTS, ROWS, FFW), jnp.float32)
    return noise * scales[:, None, :] * (2.0 / math.sqrt(FFW))


def draw_hidden(key, part):
    return hidden_values(key).astype(jnp.bfloat16)


def draw_val_grad(key, part):
    powers = jax.random.uniform(jax.random.fold_in(key, 7303), (D,), jnp.float32, -2.0, 2.0)
    sizes = jnp.exp(jax.random.uniform(jax.random.fold_in(key, 7304), (D,), jnp.float32, math.log(0.03), 0.0))
    logs = jnp.log(unit_scales(key))
    profile = jnp.exp(logs[:, :, None] * powers[None, None, :])
    profile = profile / jnp.sqrt(jnp.mean(profile * profile, axis=1, keepdims=True))
    noise = jax.random.truncated_normal(jax.random.fold_in(key, 7305), -2.5, 2.5, (EXPERTS, FFW, D), jnp.float32)
    values = noise * profile
    values = values * sizes[None, None, :]
    return jnp.clip(values, -8.0, 8.0).astype(jnp.bfloat16)


def levels(key, dims, shards, smallest, top_value):
    def one(position, parts):
        heights = jax.random.uniform(jax.random.fold_in(jax.random.fold_in(key, 6), position), (parts,), jnp.float32, smallest / len(shards), top_value / len(shards))
        return jnp.repeat(jnp.exp(heights), dims[position] // parts).reshape((-1,) + (1,) * (len(dims) - position - 1))

    factor_of = one(*shards[0])
    for cut in shards[1:]:
        factor_of = factor_of * one(*cut)
    return factor_of


def assign_block(rng, own, number, rows, amount, top, bound, slope):
    ranking = jax.random.permutation(rng, amount)
    crowded, usual = load_shares(amount, rows * top, bound, slope, True), load_shares(amount, rows * top, bound, slope, False)
    places = jnp.arange(amount)

    def named(tallies, rotation):
        used = int((tallies > 0).sum())
        fixed = max(1, used // 4)
        shifted = fixed + (places - fixed + rotation * (used - fixed)) % max(1, amount - fixed)
        return jnp.zeros((amount,), jnp.int32).at[ranking[jnp.where(places < fixed, places, shifted)]].set(jnp.asarray(tallies, jnp.int32))

    tallies = jnp.where(number % 4 == 0, named(crowded, number // 4), named(usual, number - number // 4 - 1))
    mixed = jax.random.permutation(jax.random.fold_in(own, 3), amount)
    donor, receiver = mixed[0:amount // 2 * 2:2], mixed[1:amount // 2 * 2:2]
    room = jnp.minimum(tallies[donor] - 1, bound - tallies[receiver]) // 2
    room = jnp.where((donor == ranking[0]) | (receiver == ranking[0]) | (tallies[receiver] == 0), 0, jnp.maximum(room, 0))
    shifted = jax.random.randint(jax.random.fold_in(own, 4), (amount // 2,), 0, 1 << 20) % (room + 1)
    tallies = tallies.at[donor].add(-shifted).at[receiver].add(shifted)
    members = jnp.searchsorted(jnp.cumsum(tallies), jnp.arange(rows * top), side="right").astype(jnp.int32)
    listing = members.reshape(top, rows).T
    listing = listing[jax.random.permutation(jax.random.fold_in(own, 1), rows)]
    rotation = jax.random.randint(jax.random.fold_in(own, 2), (rows, 1), 0, top)
    return jnp.take_along_axis(listing, (jnp.arange(top)[None, :] + rotation) % top, axis=1)


def load_shares(amount, total, bound, slope, full):
    portions = [(1 << 20) // math.isqrt(grade ** slope) + 1 for grade in range(1, amount + 1)]
    largest = bound if full else min(bound, max(-(-total // amount), total * portions[0] // sum(portions)))
    least = 1 if total - largest >= amount - 1 else 0
    holding, rest = [largest] + [least] * (amount - 1), total - largest - least * (amount - 1)
    while rest > 0:
        movable = [i for i in range(1, amount) if holding[i] < largest] or [i for i in range(1, amount) if holding[i] < bound]
        pool, budget = sum([portions[i] for i in movable]), rest
        for i in movable:
            extra = min(bound - holding[i], max(1, budget * portions[i] // pool), rest)
            holding[i] = holding[i] + extra
            rest = rest - extra
    return np.array(holding)


def gaussian(key, shape, deviation, most, split=(), held_as=jnp.bfloat16):
    result = jax.random.normal(key, shape, jnp.float32) * deviation
    if len(split) > 0:
        result = levels(key, shape, split, -0.22, 0.18) * result
    return jnp.clip(result, min=-most, max=most).astype(held_as)


def setup_inputs(seed: int = 0) -> dict:
    key_of = jax.random.split(jax.random.key(seed), 8)
    hidden = draw_hidden(jax.random.fold_in(key_of[7], 71), 0)
    expert_ids_keys = jax.random.split(jax.random.fold_in(key_of[1], 1), TOKENS // TOK_DEV)
    expert_ids_turns = jax.random.permutation(jax.random.fold_in(key_of[1], 3), TOKENS // TOK_DEV)
    expert_ids = jax.vmap(lambda own, number: assign_block(jax.random.fold_in(key_of[1], 2), own, number, TOK_DEV, EXPERTS, TOP, CAP, 2))(expert_ids_keys, expert_ids_turns).reshape((TOKENS, TOP))
    gate_weights = jnp.clip(0.2 + 0.8 * jax.random.uniform(key_of[2], (TOKENS, TOP), jnp.float32) ** levels(key_of[2], (TOKENS, TOP), ((0, 128),), -0.2, 0.2), 0.2, 1.0)
    loss_weight = jnp.clip(jnp.exp(math.log(3.0) - 2.3025851 * jax.random.uniform(key_of[3], (TOKENS,), jnp.float32) ** levels(key_of[3], (TOKENS,), ((0, 128),), -0.2, 0.2)), 0.3, 3.0)
    decay = jnp.clip(jnp.exp(jax.random.uniform(key_of[4], (1,), jnp.float32, math.log(0.2), math.log(0.6))), 0.2, 0.6)
    val_grad = draw_val_grad(jax.random.fold_in(key_of[7], 71), 0)
    down_weight = gaussian(key_of[6], (EXPERTS, FFW, D), FFW ** -0.5, 0.0625, ((0, 8), (1, 16)))
    return {"hidden": hidden, "expert_ids": expert_ids, "gate_weights": gate_weights, "loss_weight": loss_weight, "decay": decay, "val_grad": val_grad, "down_weight": down_weight}


def slot_rows(expert_ids):
    blocks = expert_ids.reshape(-1, TOK_DEV * TOP)
    labels = jnp.arange(EXPERTS, dtype=jnp.int32)
    onehot = (blocks[:, :, None] == labels[None, None, :]).astype(jnp.int32)
    earlier = jnp.cumsum(onehot, axis=1) - onehot
    slots = lax.optimization_barrier(jnp.sum(earlier * onehot, axis=2)).reshape(-1, TOP)
    owner = jnp.arange(TOKENS, dtype=jnp.int32) // TOK_DEV
    base = (owner % N_FSDP * N_EXPERT + owner // N_FSDP) * CAP
    return (base[:, None] + slots).astype(jnp.int32)

def hessian_product(direction, hidden, expert_ids, rows, gate_weights, loss_weight, decay):
    rounded = direction.astype(jnp.bfloat16)

    def forward(operands):
        return jnp.dot(operands[0], operands[1], preferred_element_type=jnp.float32)
    outputs = lax.map(forward, (hidden, rounded))
    picked = outputs[expert_ids, rows]
    mixed = lax.optimization_barrier(jnp.sum(gate_weights[:, :, None] * picked, axis=1))
    scaled = loss_weight[:, None] * mixed
    sent = (gate_weights[:, :, None] * scaled[:, None, :]).astype(jnp.bfloat16)
    placed = jnp.zeros(outputs.shape, jnp.bfloat16).at[expert_ids, rows].set(sent)

    def backward(operands):
        return jnp.dot(operands[0].T, operands[1], preferred_element_type=jnp.float32)
    return lax.map(backward, (hidden, placed)) + decay[0] * direction

def reference(hidden, expert_ids, gate_weights, loss_weight, decay, val_grad, down_weight):
    rows = slot_rows(expert_ids)
    right = val_grad.astype(jnp.float32)
    solution = jnp.zeros_like(right)
    residual = right
    direction = right
    norm_now = jnp.sum(residual * residual)
    for iteration in range(ITERS):
        image = hessian_product(direction, hidden, expert_ids, rows, gate_weights, loss_weight, decay)
        alpha = norm_now / jnp.sum(direction * image)
        solution = solution + alpha * direction
        residual = residual - alpha * image
        if iteration + 1 < ITERS:
            norm_next = jnp.sum(residual * residual)
            direction = residual + norm_next / norm_now * direction
            norm_now = norm_next
    along = jnp.sum(down_weight.astype(jnp.float32) * solution)
    hyper = -along / math.sqrt(EXPERTS * D)
    return (solution, jnp.reshape(hyper, (1,)).astype(jnp.float32))
```

```python
import functools
import math

import jax
import jax.numpy as jnp
from jax import lax
from jax.experimental import pallas as pl
from jax.experimental.pallas import tpu as pltpu
from jax.sharding import Mesh
from jax.sharding import PartitionSpec as P

EXPERT_FSDP = ("expert_0", "expert_1", "fsdp_0", "fsdp_1")
EXPERT = ("expert_0", "expert_1")
FSDP = ("fsdp_0", "fsdp_1")
PARAMS = dict(vmem_limit_bytes=48 * 1024 * 1024)


def shift(array, axis, amount):
    size = lax.axis_size(axis)
    return lax.ppermute(array, axis, [(i, (i + amount) % size) for i in range(size)])


def pick(array, index):
    return lax.dynamic_index_in_dim(array, index, 0, keepdims=False)


def exchange_axis(blocks, axis):
    size = lax.axis_size(axis)
    me = lax.axis_index(axis)
    received = [(me, pick(blocks, me))]
    for step in range(1, size):
        sent = pick(blocks, (me + step) % size)
        received.append(((me - step) % size, shift(sent, axis, step)))
    return received


def placed(received, size):
    first = received[0][1]
    array = jnp.zeros((size,) + first.shape, first.dtype)
    for index, block in received:
        array = lax.dynamic_update_index_in_dim(array, block, index, 0)
    return array


def gather_axis(block, axis):
    size = lax.axis_size(axis)
    me = lax.axis_index(axis)
    received = [(me, block)]
    for step in range(1, size):
        received.append(((me - step) % size, shift(block, axis, step)))
    return placed(received, size)


def expert_exchange(rows):
    outer, inner = lax.axis_size("expert_0"), lax.axis_size("expert_1")
    block = rows.shape[0] // (outer * inner)
    blocks = rows.reshape((outer, inner, block) + rows.shape[1:]).swapaxes(0, 1)
    by_core = placed(exchange_axis(blocks, "expert_1"), inner)
    by_chip = placed(exchange_axis(by_core.swapaxes(0, 1), "expert_0"), outer)
    return by_chip.reshape(rows.shape)


def gram(hidden):
    partial = lax.dot_general(
        hidden, hidden, (((1,), (1,)), ((), ())), preferred_element_type=jnp.float32
    )
    size = partial.shape[0]
    block = partial
    for axis in FSDP:
        parts = lax.axis_size(axis)
        block = block.reshape(parts, -1, size).astype(jnp.bfloat16)
        terms = exchange_axis(block, axis)
        block = sum(term.astype(jnp.float32) for _, term in terms)
    block = block.astype(jnp.bfloat16)
    for axis in FSDP[::-1]:
        block = gather_axis(block, axis).reshape(-1, size)
    return block


def all_sum(values):
    for axis in EXPERT_FSDP[::-1]:
        size = lax.axis_size(axis)
        values = sum([values] + [shift(values, axis, step) for step in range(1, size)])
    return values


def gate_tables(packed, experts, capacity):
    blocks, tokens, _ = packed.shape
    top = (packed.shape[2] - 1) // 2
    ids = packed[:, :, :top].reshape(blocks, tokens * top).astype(jnp.int32)
    gates = packed[:, :, top : 2 * top].reshape(blocks, tokens * top)
    same = ids[:, :, None] == ids[:, None, :]
    order = jnp.arange(tokens * top)
    earlier = order[None, :] < order[:, None]
    slots = jnp.sum((same & earlier[None]).astype(jnp.int32), axis=2)
    column = ids * (blocks * capacity) + jnp.arange(blocks)[:, None] * capacity + slots
    columns = jnp.arange(experts * blocks * capacity)
    hits = column[:, :, None] == columns[None, None, :]
    weighted = jnp.where(hits, gates[:, :, None], 0.0)
    weighted = weighted.reshape(blocks * tokens, top, -1)
    return jnp.sum(weighted, axis=1), packed[:, :, 2 * top].reshape(-1)


def outputs_kernel(hidden_ref, side_ref, out_ref):
    out_ref[0] = jnp.dot(hidden_ref[...], side_ref[...], preferred_element_type=jnp.float32)


def expert_outputs(hidden, side, parts):
    rows, depth = hidden.shape
    width = side.shape[1] // parts
    return pl.pallas_call(
        outputs_kernel,
        grid=(parts,),
        in_specs=[
            pl.BlockSpec((rows, depth), lambda i: (0, 0)),
            pl.BlockSpec((depth, width), lambda i: (0, i)),
        ],
        out_specs=pl.BlockSpec((1, rows, width), lambda i: (i, 0, 0)),
        out_shape=jax.ShapeDtypeStruct((parts, rows, width), jnp.float32),
        compiler_params=pltpu.CompilerParams(**PARAMS),
        cost_estimate=pl.CostEstimate(
            flops=2 * rows * depth * side.shape[1],
            bytes_accessed=4 * rows * side.shape[1],
            transcendentals=0,
        ),
        name="expert_outputs",
    )(hidden, side)


def finish_kernel(coef_ref, hidden_ref, tangent_ref, side_ref, target_ref, out_ref, along_ref):
    image = jnp.dot(hidden_ref[...], tangent_ref[0], preferred_element_type=jnp.float32)
    side = side_ref[...].astype(jnp.float32)
    out_ref[...] = coef_ref[0] * side + coef_ref[1] * image
    product = target_ref[...].astype(jnp.float32) * image
    along_ref[0] = jnp.sum(product.reshape(-1, 8, product.shape[1]), axis=0)


def finish(coefs, hidden_t, tangents, side, target):
    parts, rows, width = tangents.shape
    depth = hidden_t.shape[0]
    return pl.pallas_call(
        finish_kernel,
        grid=(parts,),
        in_specs=[
            pl.BlockSpec(memory_space=pltpu.SMEM),
            pl.BlockSpec((depth, rows), lambda i: (0, 0)),
            pl.BlockSpec((1, rows, width), lambda i: (i, 0, 0)),
            pl.BlockSpec((depth, width), lambda i: (0, i)),
            pl.BlockSpec((depth, width), lambda i: (0, i)),
        ],
        out_specs=[
            pl.BlockSpec((depth, width), lambda i: (0, i)),
            pl.BlockSpec((1, 8, width), lambda i: (i, 0, 0)),
        ],
        out_shape=[
            jax.ShapeDtypeStruct((depth, parts * width), jnp.float32),
            jax.ShapeDtypeStruct((parts, 8, width), jnp.float32),
        ],
        compiler_params=pltpu.CompilerParams(**PARAMS),
        cost_estimate=pl.CostEstimate(
            flops=2 * rows * depth * parts * width,
            bytes_accessed=10 * depth * parts * width,
            transcendentals=0,
        ),
        name="finish",
    )(coefs, hidden_t, tangents, side, target)


def mix(table, rows):
    return jnp.dot(
        table, rows, precision=lax.Precision.HIGHEST, preferred_element_type=jnp.float32
    )


def local(hidden, expert_ids, gate_weights, loss_weight, decay, val_grad, down_weight):
    n_expert = lax.axis_size(EXPERT)
    n_fsdp = lax.axis_size(FSDP)
    capacity = hidden.shape[1] // (n_expert * n_fsdp)
    tokens, top = expert_ids.shape
    rate = decay[0]
    acts, side, target = hidden[0], val_grad[0], down_weight[0]

    partial = expert_outputs(acts, side, n_fsdp)
    rows, width = partial.shape[1:]
    summed = lax.psum_scatter(
        partial.reshape(n_fsdp * rows, width), FSDP, scatter_dimension=0, tiled=True
    )

    packed = jnp.concatenate(
        [expert_ids.astype(jnp.float32), gate_weights, loss_weight[:, None]], axis=1
    )
    share = n_fsdp // n_expert
    everyone = lax.all_gather(packed, EXPERT_FSDP).reshape(n_expert, n_fsdp, tokens, -1)
    mine = lax.dynamic_slice_in_dim(everyone, lax.axis_index(EXPERT) * share, share, 1)
    mine = mine.swapaxes(0, 1).reshape(share * n_expert, tokens, -1)
    table, weights = gate_tables(mine, n_expert, capacity)
    kernel_matrix = gram(acts)
    wide = side.astype(jnp.float32)
    norm = jnp.sum(wide * wide)
    fixed = jnp.sum(target.astype(jnp.float32) * wide)

    arrived = expert_exchange(summed)
    mixed = mix(table, arrived)
    scaled = weights[:, None] * mixed
    leaving = mix(table.T, scaled).astype(jnp.bfloat16)
    returned = expert_exchange(leaving)
    tangents = lax.all_gather(returned, FSDP, axis=0, tiled=True)

    second = jnp.dot(kernel_matrix, returned, preferred_element_type=jnp.float32)
    square = jnp.sum(second * returned.astype(jnp.float32))
    again = mix(table, expert_exchange(second.astype(jnp.bfloat16)).astype(jnp.float32))
    parts = jnp.stack(
        [
            norm,
            jnp.sum(scaled * mixed),
            square,
            jnp.sum(weights[:, None] * again * again),
            fixed,
        ]
    )
    bb, bg, gg, ghg, wb = all_sum(parts)
    alpha = bb / (bg + rate * bb)
    lean = bg / bb
    across = gg - bg * lean
    fresh = alpha * alpha * across
    beta = fresh / bb
    bent = ghg - 2.0 * lean * gg + lean * lean * bg
    curve = alpha * alpha * (bent + rate * across) - beta * fresh / alpha
    step = fresh / curve
    keep = alpha + step * (beta + alpha * lean)
    move = -step * alpha

    result, along = finish(
        jnp.stack([keep, move]), acts.T, tangents.reshape(n_fsdp, rows, width), side, target
    )
    wg = all_sum(jnp.sum(along).reshape(1))[0]
    hyper = -(keep * wb + move * wg) / math.sqrt(n_expert * side.shape[1])
    return (result[None], jnp.reshape(hyper, (1,)))


def solution(mesh):
    finer = Mesh(mesh.devices.reshape(4, 2, 4, 4), EXPERT_FSDP)
    specs = (
        P(EXPERT, None, FSDP),
        P(EXPERT_FSDP, None),
        P(EXPERT_FSDP, None),
        P(EXPERT_FSDP),
        P(),
        P(EXPERT, FSDP, None),
        P(EXPERT, FSDP, None),
    )
    return jax.shard_map(
        local, mesh=finer, in_specs=specs, out_specs=(P(EXPERT, FSDP, None), P()), check_vma=False
    )
```

```python
import math

import jax
import jax.numpy as jnp
from jax import lax
from jax.experimental import pallas as pl
from jax.experimental.pallas import tpu as pltpu
from jax.sharding import Mesh
from jax.sharding import PartitionSpec as P

EXPERT_FSDP = ("expert_0", "expert_1", "fsdp_0", "fsdp_1")
EXPERT = ("expert_0", "expert_1")
FSDP = ("fsdp_0", "fsdp_1")
PARAMS = dict(vmem_limit_bytes=60 * 1024 * 1024)
CHUNKS = 1
SPAN = 512


def shift(array, axis, amount):
    size = lax.axis_size(axis)
    return lax.ppermute(array, axis, [(i, (i + amount) % size) for i in range(size)])


def pick(array, index):
    return lax.dynamic_index_in_dim(array, index, 0, keepdims=False)


def exchange_axis(blocks, axis):
    size = lax.axis_size(axis)
    me = lax.axis_index(axis)
    received = [(me, pick(blocks, me))]
    for step in range(1, size):
        sent = pick(blocks, (me + step) % size)
        received.append(((me - step) % size, shift(sent, axis, step)))
    return received


def gather_axis(block, axis):
    size = lax.axis_size(axis)
    me = lax.axis_index(axis)
    array = jnp.zeros((size,) + block.shape, block.dtype)
    array = lax.dynamic_update_index_in_dim(array, block, me, 0)
    for step in range(1, size):
        arrived = shift(block, axis, step)
        array = lax.dynamic_update_index_in_dim(array, arrived, (me - step) % size, 0)
    return array


def relative(rows):
    outer, inner = lax.axis_size("expert_0"), lax.axis_size("expert_1")
    chip, core = lax.axis_index("expert_0"), lax.axis_index("expert_1")
    blocks = rows.reshape((outer, inner, -1) + rows.shape[1:])
    blocks = jnp.where(core == 0, blocks, blocks[:, ::-1])
    twice = jnp.concatenate([blocks, blocks], axis=0)
    return lax.dynamic_slice_in_dim(twice, chip, outer, 0).reshape(rows.shape)


def expert_exchange(rows, sign):
    outer, inner = lax.axis_size("expert_0"), lax.axis_size("expert_1")
    block = rows.shape[0] // (outer * inner)
    blocks = rows.reshape((outer, inner, block) + rows.shape[1:])
    other = shift(blocks[:, 1], "expert_1", 1)
    out = []
    for step in range(outer):
        pair = jnp.stack([blocks[step, 0], other[step]])
        out.append(shift(pair, "expert_0", sign * step) if step else pair)
    return jnp.concatenate(out).reshape(rows.shape)


def gram(hidden):
    partial = lax.dot_general(
        hidden, hidden, (((1,), (1,)), ((), ())), preferred_element_type=jnp.float32
    )
    size = partial.shape[0]
    block = partial
    for axis in FSDP:
        parts = lax.axis_size(axis)
        block = block.reshape(parts, -1, size).astype(jnp.bfloat16)
        terms = exchange_axis(block, axis)
        block = sum(term.astype(jnp.float32) for _, term in terms)
    block = block.astype(jnp.bfloat16)
    for axis in FSDP[::-1]:
        block = gather_axis(block, axis).reshape(-1, size)
    return block


def all_sum(values):
    for axis in EXPERT_FSDP[::-1]:
        size = lax.axis_size(axis)
        values = sum([values] + [shift(values, axis, step) for step in range(1, size)])
    return values


def gate_tables(packed, experts, capacity):
    blocks, tokens, _ = packed.shape
    top = (packed.shape[2] - 1) // 2
    outer, inner = lax.axis_size("expert_0"), lax.axis_size("expert_1")
    chip, core = lax.axis_index("expert_0"), lax.axis_index("expert_1")
    ids = packed[:, :, :top].reshape(blocks, tokens * top).astype(jnp.int32)
    gates = packed[:, :, top : 2 * top].reshape(blocks, tokens * top)
    same = ids[:, :, None] == ids[:, None, :]
    order = jnp.arange(tokens * top)
    earlier = order[None, :] < order[:, None]
    slots = jnp.sum((same & earlier[None]).astype(jnp.int32), axis=2)
    places = (chip - ids // inner) % outer * inner + (core - ids % inner) % inner
    column = places * (blocks * capacity) + jnp.arange(blocks)[:, None] * capacity + slots
    columns = jnp.arange(experts * blocks * capacity)
    hits = column[:, :, None] == columns[None, None, :]
    weighted = jnp.where(hits, gates[:, :, None], 0.0)
    weighted = weighted.reshape(blocks * tokens, top, -1)
    return jnp.sum(weighted, axis=1), packed[:, :, 2 * top].reshape(-1)


def outputs_kernel(hidden_ref, side_ref, out_ref):
    group, rows, width = out_ref.shape
    tile = rows // 3

    @pl.loop(0, 3)
    def _(i):
        part = pl.ds(pl.multiple_of(i * tile, tile), tile)
        product = jnp.dot(hidden_ref[part, :], side_ref[...], preferred_element_type=jnp.float32)
        for k in range(group):
            out_ref[k, part, :] = product[:, k * width : (k + 1) * width]


def expert_outputs(hidden, side, parts, chunk):
    rows, depth = hidden.shape
    width = side.shape[1] // parts // CHUNKS
    group = SPAN // width
    steps = parts // group
    return pl.pallas_call(
        outputs_kernel,
        grid=(steps,),
        in_specs=[
            pl.BlockSpec((rows, depth), lambda i: (0, 0)),
            pl.BlockSpec((depth, group * width), lambda i: (0, chunk * steps + i)),
        ],
        out_specs=pl.BlockSpec((group, rows, width), lambda i: (i, 0, 0)),
        out_shape=jax.ShapeDtypeStruct((parts, rows, width), jnp.float32),
        compiler_params=pltpu.CompilerParams(**PARAMS),
        cost_estimate=pl.CostEstimate(
            flops=2 * rows * depth * parts * width,
            bytes_accessed=4 * rows * parts * width,
            transcendentals=0,
        ),
        name="expert_outputs",
    )(hidden, side)


def finish_kernel(coef_ref, hidden_ref, tangent_ref, side_ref, held_ref, out_ref):
    group = tangent_ref.shape[0]
    tangents = jnp.concatenate([tangent_ref[k] for k in range(group)], axis=1)
    image = jnp.dot(hidden_ref[...], tangents, preferred_element_type=jnp.float32)
    out_ref[...] = coef_ref[0] * side_ref[...].astype(jnp.float32) + coef_ref[1] * image


def finish(coefs, hidden_t, tangents, side, held, chunk):
    parts, rows, width = tangents.shape
    depth = hidden_t.shape[0]
    group = SPAN // width
    steps = parts // group
    column = pl.BlockSpec((depth, group * width), lambda i: (0, chunk * steps + i))
    specs = [
        pl.BlockSpec(memory_space=pltpu.SMEM),
        pl.BlockSpec((depth, rows), lambda i: (0, 0)),
        pl.BlockSpec((group, rows, width), lambda i: (i, 0, 0)),
        column,
    ]
    args = [coefs, hidden_t, tangents, side]
    kernel = lambda c, h, t, s, o: finish_kernel(c, h, t, s, None, o)
    aliases = {}
    if held is not None:
        kernel = finish_kernel
        specs.append(pl.BlockSpec(memory_space=pl.ANY))
        args.append(held)
        aliases = {4: 0}
    return pl.pallas_call(
        kernel,
        grid=(steps,),
        in_specs=specs,
        out_specs=column,
        out_shape=jax.ShapeDtypeStruct(side.shape, jnp.float32),
        input_output_aliases=aliases,
        compiler_params=pltpu.CompilerParams(**PARAMS),
        cost_estimate=pl.CostEstimate(
            flops=2 * rows * depth * parts * width,
            bytes_accessed=8 * depth * parts * width,
            transcendentals=0,
        ),
        name="finish",
    )(*args)


def mix(table, rows):
    return jnp.dot(
        table, rows, precision=lax.Precision.HIGHEST, preferred_element_type=jnp.float32
    )


def local(hidden, expert_ids, gate_weights, loss_weight, decay, val_grad, down_weight):
    n_expert = lax.axis_size(EXPERT)
    n_fsdp = lax.axis_size(FSDP)
    capacity = hidden.shape[1] // (n_expert * n_fsdp)
    tokens, top = expert_ids.shape
    rate = decay[0]
    side, target = val_grad[0], down_weight[0]
    acts = relative(hidden[0])
    rows = acts.shape[0]

    summed = []
    for chunk in range(CHUNKS):
        partial = expert_outputs(acts, side, n_fsdp, chunk)
        summed.append(
            lax.psum_scatter(
                partial.reshape(n_fsdp * rows, -1), FSDP, scatter_dimension=0, tiled=True
            )
        )

    packed = jnp.concatenate(
        [expert_ids.astype(jnp.float32), gate_weights, loss_weight[:, None]], axis=1
    )
    share = n_fsdp // n_expert
    for axis in EXPERT_FSDP[::-1]:
        packed = gather_axis(packed, axis)
    everyone = packed.reshape(n_expert, n_fsdp, tokens, -1)
    mine = lax.dynamic_slice_in_dim(everyone, lax.axis_index(EXPERT) * share, share, 1)
    mine = mine.swapaxes(0, 1).reshape(share * n_expert, tokens, -1)
    table, weights = gate_tables(mine, n_expert, capacity)
    kernel_matrix = gram(acts)
    wide = side.astype(jnp.float32)
    norm = jnp.sum(wide * wide)
    fixed = jnp.sum(target.astype(jnp.float32) * wide)
    targets = [expert_outputs(acts, target, n_fsdp, chunk) for chunk in range(CHUNKS)]
    acts_t = acts.T
    summed[0], table, weights, kernel_matrix, norm, fixed, targets, acts_t = (
        lax.optimization_barrier(
            (summed[0], table, weights, kernel_matrix, norm, fixed, targets, acts_t)
        )
    )

    returned, tangents = [], []
    bg = gg = ghg = wg = 0.0
    for chunk in range(CHUNKS):
        mixed = mix(table, expert_exchange(summed[chunk], 1))
        scaled = weights[:, None] * mixed
        bg += jnp.sum(scaled * mixed)
        leaving = mix(table.T, scaled).astype(jnp.bfloat16)
        returned.append(expert_exchange(leaving, -1))
        gathered = lax.all_gather(returned[chunk], FSDP, axis=0, tiled=True)
        tangents.append(gathered.reshape(n_fsdp, rows, -1))
    for chunk in range(CHUNKS):
        second = jnp.dot(kernel_matrix, returned[chunk], preferred_element_type=jnp.float32)
        gg += jnp.sum(second * returned[chunk].astype(jnp.float32))
        exchanged = expert_exchange(second.astype(jnp.bfloat16), 1)
        again = mix(table, exchanged.astype(jnp.float32))
        ghg += jnp.sum(weights[:, None] * again * again)
    bb, bg, gg, ghg, wb = all_sum(jnp.stack([norm, bg, gg, ghg, fixed]))
    alpha = bb / (bg + rate * bb)
    lean = bg / bb
    across = gg - bg * lean
    fresh = alpha * alpha * across
    beta = fresh / bb
    bent = ghg - 2.0 * lean * gg + lean * lean * bg
    curve = alpha * alpha * (bent + rate * across) - beta * fresh / alpha
    step = fresh / curve
    keep = alpha + step * (beta + alpha * lean)
    move = -step * alpha

    for chunk in range(CHUNKS):
        wg += jnp.sum(targets[chunk] * tangents[chunk].astype(jnp.float32))
    wg = all_sum(jnp.reshape(wg, (1,)))[0]
    result = None
    for chunk in range(CHUNKS):
        result = finish(jnp.stack([keep, move]), acts_t, tangents[chunk], side, result, chunk)
    hyper = -(keep * wb + move * wg) / math.sqrt(n_expert * side.shape[1])
    return (result[None], jnp.reshape(hyper, (1,)))


def solution(mesh):
    finer = Mesh(mesh.devices.reshape(4, 2, 4, 4), EXPERT_FSDP)
    specs = (
        P(EXPERT, None, FSDP),
        P(EXPERT_FSDP, None),
        P(EXPERT_FSDP, None),
        P(EXPERT_FSDP),
        P(),
        P(EXPERT, FSDP, None),
        P(EXPERT, FSDP, None),
    )
    return jax.shard_map(
        local, mesh=finer, in_specs=specs, out_specs=(P(EXPERT, FSDP, None), P()), check_vma=False
    )
```

```python
import math

import jax
import jax.numpy as jnp
from jax import lax
from jax.experimental import pallas as pl
from jax.experimental.pallas import tpu as pltpu
from jax.sharding import Mesh
from jax.sharding import PartitionSpec as P

EXPERT_FSDP = ("expert_0", "expert_1", "fsdp_0", "fsdp_1")
EXPERT = ("expert_0", "expert_1")
FSDP = ("fsdp_0", "fsdp_1")
PARAMS = dict(vmem_limit_bytes=60 * 1024 * 1024)
LANES = 128


def shift(array, axis, amount):
    size = lax.axis_size(axis)
    return lax.ppermute(array, axis, [(i, (i + amount) % size) for i in range(size)])


def pick(array, index):
    return lax.dynamic_index_in_dim(array, index, 0, keepdims=False)


def ring_reduce(blocks, axis):
    own, near, far, back = blocks
    half = far.shape[0] // 2
    far_up = shift(far[:half], axis, 1)
    far_down = shift(far[half:], axis, -1)
    near_up = shift(near[half:], axis, 1)
    back_down = shift(back[:half], axis, -1)
    last_up = shift(near[:half] + far_up, axis, 1)
    last_down = shift(back[half:] + far_down, axis, -1)
    return own[:half] + back_down + last_up, own[half:] + near_up + last_down


def short_reduce(blocks, axis):
    own, near, far, back = blocks
    half = far.shape[0] // 2
    far_up = shift(far[:half], axis, 1)
    far_down = shift(far[half:], axis, -1)
    near_up = shift(jnp.concatenate([near[:half] + far_up, near[half:]]), axis, 1)
    back_down = shift(jnp.concatenate([back[:half], back[half:] + far_down]), axis, -1)
    return own + near_up + back_down


def relative(rows):
    outer, inner = lax.axis_size("expert_0"), lax.axis_size("expert_1")
    chip, core = lax.axis_index("expert_0"), lax.axis_index("expert_1")
    blocks = rows.reshape((outer, inner, -1) + rows.shape[1:])
    blocks = jnp.where(core == 0, blocks, blocks[:, ::-1])
    twice = jnp.concatenate([blocks, blocks], axis=0)
    return lax.dynamic_slice_in_dim(twice, chip, outer, 0).reshape(rows.shape)


def expert_exchange(rows, sign):
    outer, inner = lax.axis_size("expert_0"), lax.axis_size("expert_1")
    block = rows.shape[0] // (outer * inner)
    blocks = rows.reshape((outer, inner, block) + rows.shape[1:])
    other = shift(blocks[:, 1], "expert_1", 1)
    out = []
    for step in range(outer):
        pair = jnp.stack([blocks[step, 0], other[step]])
        out.append(shift(pair, "expert_0", sign * step) if step else pair)
    return jnp.concatenate(out).reshape(rows.shape)


def all_sum(values):
    for axis in EXPERT_FSDP[::-1]:
        size = lax.axis_size(axis)
        values = sum([values] + [shift(values, axis, step) for step in range(1, size)])
    return values


def direct_sum(values):
    size = lax.axis_size(EXPERT_FSDP)
    copies = jnp.broadcast_to(values[None], (size,) + values.shape)
    return jnp.sum(
        lax.all_to_all(copies, EXPERT_FSDP, split_axis=0, concat_axis=0, tiled=True), axis=0
    )


def gate_tables(packed, experts, capacity):
    blocks, tokens, _ = packed.shape
    top = (packed.shape[2] - 1) // 2
    outer, inner = lax.axis_size("expert_0"), lax.axis_size("expert_1")
    chip, core = lax.axis_index("expert_0"), lax.axis_index("expert_1")
    ids = packed[:, :, :top].reshape(blocks, tokens * top).astype(jnp.int32)
    gates = packed[:, :, top : 2 * top].reshape(blocks, tokens * top)
    same = ids[:, :, None] == ids[:, None, :]
    order = jnp.arange(tokens * top)
    earlier = order[None, :] < order[:, None]
    slots = jnp.sum((same & earlier[None]).astype(jnp.int32), axis=2)
    places = (chip - ids // inner) % outer * inner + (core - ids % inner) % inner
    column = places * (blocks * capacity) + jnp.arange(blocks)[:, None] * capacity + slots
    columns = jnp.arange(experts * blocks * capacity)
    hits = column[:, :, None] == columns[None, None, :]
    weighted = jnp.where(hits, gates[:, :, None], 0.0)
    weighted = weighted.reshape(blocks * tokens, top, -1)
    return jnp.sum(weighted, axis=1), packed[:, :, 2 * top].reshape(-1)


def column_of(row, column, place_ref):
    return (place_ref[0] + row) % 4 * 4 + (place_ref[1] + column) % 4


def outputs_kernel(place_ref, hidden_ref, left_ref, right_ref, x_ref, y_ref, norm_ref):
    half, width = x_ref.shape[2:]
    side = jnp.concatenate([left_ref[...], right_ref[...]], axis=1)
    tile = half // 2
    for part in range(2):

        @pl.loop(0, 2)
        def _(i):
            rows = pl.ds(pl.multiple_of(i * tile, tile), tile)
            source = pl.ds(pl.multiple_of(i * tile + part * half, tile), tile)
            product = jnp.dot(hidden_ref[source, :], side, preferred_element_type=jnp.float32)
            for k in range(2):
                piece = product[:, k * width : (k + 1) * width]
                if part == 0:
                    x_ref[k, 0, rows, :] = piece
                else:
                    y_ref[0, k, rows, :] = piece

    wide = side.astype(jnp.float32)
    square = wide * wide
    norm_ref[0] = jnp.sum(square.reshape(-1, 8, square.shape[1]), axis=0)


def expert_outputs(place, hidden, side):
    rows, depth = hidden.shape
    width = side.shape[1] // 16
    half = rows // 2
    out = jax.ShapeDtypeStruct((4, 4, half, width), jnp.float32)
    return pl.pallas_call(
        outputs_kernel,
        grid_spec=pltpu.PrefetchScalarGridSpec(
            num_scalar_prefetch=1,
            grid=(8,),
            in_specs=[
                pl.BlockSpec((rows, depth), lambda i, p: (0, 0)),
                pl.BlockSpec((depth, width), lambda i, p: (0, column_of(i // 2, i % 2 * 2, p))),
                pl.BlockSpec(
                    (depth, width), lambda i, p: (0, column_of(i // 2, i % 2 * 2 + 1, p))
                ),
            ],
            out_specs=[
                pl.BlockSpec((2, 1, half, width), lambda i, p: (i % 2, i // 2, 0, 0)),
                pl.BlockSpec((1, 2, half, width), lambda i, p: (i // 2, i % 2, 0, 0)),
                pl.BlockSpec((1, 8, 2 * width), lambda i, p: (i, 0, 0)),
            ],
        ),
        out_shape=[out, out, jax.ShapeDtypeStruct((8, 8, 2 * width), jnp.float32)],
        compiler_params=pltpu.CompilerParams(**PARAMS),
        cost_estimate=pl.CostEstimate(
            flops=2 * rows * depth * side.shape[1],
            bytes_accessed=4 * rows * side.shape[1],
            transcendentals=0,
        ),
        name="expert_outputs",
    )(place, hidden, side, side)


def finish_kernel(
    coef_ref, hidden_ref, tangent_ref, side_ref, target_ref, out_ref, image_ref, along_ref
):
    tangents = jnp.concatenate([tangent_ref[0], tangent_ref[1]], axis=1)
    tile = hidden_ref.shape[0] // 2
    image_ref[...] = jnp.zeros_like(image_ref)
    along_ref[...] = jnp.zeros_like(along_ref)

    @pl.loop(0, 2)
    def _(i):
        part = pl.ds(pl.multiple_of(i * tile, tile), tile)
        image = jnp.dot(hidden_ref[part, :], tangents, preferred_element_type=jnp.float32)
        side = side_ref[part, :].astype(jnp.float32)
        target = target_ref[part, :].astype(jnp.float32)
        out_ref[part, :] = coef_ref[0, 0] * side + coef_ref[1, 0] * image
        image_ref[0] += jnp.sum((target * image).reshape(-1, 8, image.shape[1]), axis=0)
        along_ref[0] += jnp.sum((target * side).reshape(-1, 8, image.shape[1]), axis=0)


def finish(coefs, hidden_t, tangents, side, target):
    width = tangents.shape[2]
    depth, rows = hidden_t.shape
    column = pl.BlockSpec((depth, 2 * width), lambda i: (0, i))
    sums = pl.BlockSpec((1, 8, 2 * width), lambda i: (i, 0, 0))
    sums_shape = jax.ShapeDtypeStruct((8, 8, 2 * width), jnp.float32)
    return pl.pallas_call(
        finish_kernel,
        grid=(8,),
        in_specs=[
            pl.BlockSpec(memory_space=pltpu.SMEM),
            pl.BlockSpec((depth, rows), lambda i: (0, 0)),
            pl.BlockSpec((2, rows, width), lambda i: (i, 0, 0)),
            column,
            column,
        ],
        out_specs=[column, sums, sums],
        out_shape=[jax.ShapeDtypeStruct(side.shape, jnp.float32), sums_shape, sums_shape],
        compiler_params=pltpu.CompilerParams(**PARAMS),
        cost_estimate=pl.CostEstimate(
            flops=2 * rows * depth * side.shape[1],
            bytes_accessed=12 * depth * side.shape[1],
            transcendentals=0,
        ),
        name="finish",
    )(coefs, hidden_t, tangents, side, target)


def mix(table, rows):
    return jnp.dot(
        table, rows, precision=lax.Precision.HIGHEST, preferred_element_type=jnp.float32
    )


def lanes(array):
    return jnp.sum(jnp.sum(array.reshape(-1, array.shape[-1]), axis=0).reshape(-1, LANES), axis=0)


def local(hidden, expert_ids, gate_weights, loss_weight, decay, val_grad, down_weight):
    n_expert = lax.axis_size(EXPERT)
    n_fsdp = lax.axis_size(FSDP)
    capacity = hidden.shape[1] // (n_expert * n_fsdp)
    tokens, top = expert_ids.shape
    rate = decay[0]
    side, target = val_grad[0], down_weight[0]
    acts = relative(hidden[0])
    place = jnp.stack([lax.axis_index("fsdp_0"), lax.axis_index("fsdp_1")]).astype(jnp.int32)

    partial = lax.dot_general(
        acts, acts, (((1,), (1,)), ((), ())), preferred_element_type=jnp.float32
    )
    partial, acts = lax.optimization_barrier((partial, acts))
    kernel_matrix = lax.psum(partial, FSDP)

    x_part, y_part, norm = expert_outputs(place, acts, side)
    packed = jnp.concatenate(
        [expert_ids.astype(jnp.float32), gate_weights, loss_weight[:, None]], axis=1
    )
    packed = jnp.pad(packed.reshape(1, -1), ((0, 0), (0, LANES - packed.size % LANES)))
    packed, x_part, y_part = lax.optimization_barrier((packed, x_part, y_part))
    x_mid = [block for part in ring_reduce(x_part, "fsdp_1") for block in (part[0], part[1])]
    y_mid = [block for part in ring_reduce(y_part, "fsdp_0") for block in (part[0], part[1])]
    x_sum = short_reduce(x_mid, "fsdp_0")
    y_sum = short_reduce(y_mid, "fsdp_1")

    share = n_fsdp // n_expert
    everyone = lax.all_to_all(
        jnp.broadcast_to(packed, (n_expert * n_fsdp, packed.shape[1])),
        EXPERT_FSDP,
        split_axis=0,
        concat_axis=0,
        tiled=True,
    )
    everyone = everyone.reshape(n_expert, n_fsdp, -1)
    mine = lax.dynamic_slice_in_dim(everyone, lax.axis_index(EXPERT) * share, share, 1)
    mine = mine.swapaxes(0, 1).reshape(share * n_expert, -1)[:, : tokens * (2 * top + 1)]
    table, weights = gate_tables(mine.reshape(-1, tokens, 2 * top + 1), n_expert, capacity)
    acts_t = acts.T
    summed = jnp.concatenate([x_sum, y_sum])
    summed, table, weights, acts_t = lax.optimization_barrier((summed, table, weights, acts_t))

    mixed = mix(table, expert_exchange(summed, 1))
    scaled = weights[:, None] * mixed
    leaving = mix(table.T, scaled).astype(jnp.bfloat16)
    returned = expert_exchange(leaving, -1)
    gathered = lax.all_gather(returned, FSDP, axis=0, tiled=True)
    tangents = gathered.reshape((n_fsdp,) + returned.shape)

    high = kernel_matrix.astype(jnp.bfloat16)
    low = (kernel_matrix - high.astype(jnp.float32)).astype(jnp.bfloat16)
    second = jnp.dot(high, returned, preferred_element_type=jnp.float32)
    second += jnp.dot(low, returned, preferred_element_type=jnp.float32)
    again = mix(table, expert_exchange(second.astype(jnp.bfloat16), 1).astype(jnp.float32))
    sums = jnp.stack(
        [
            lanes(norm),
            lanes(scaled * mixed),
            lanes(second * returned.astype(jnp.float32)),
            lanes(weights[:, None] * again * again),
        ]
    )
    sums = jnp.sum(all_sum(sums), axis=1, keepdims=True)
    sums = jnp.broadcast_to(sums, (sums.shape[0], LANES))
    bb, bg, gg, ghg = (sums[k] for k in range(4))
    alpha = bb / (bg + rate * bb)
    lean = bg / bb
    across = gg - bg * lean
    fresh = alpha * alpha * across
    beta = fresh / bb
    bent = ghg - 2.0 * lean * gg + lean * lean * bg
    curve = alpha * alpha * (bent + rate * across) - beta * fresh / alpha
    step = fresh / curve
    keep = alpha + step * (beta + alpha * lean)
    move = -step * alpha

    coefs = jnp.stack([keep, move])
    result, image, along = finish(coefs, acts_t, tangents, side, target)
    image, along = direct_sum(jnp.stack([lanes(image), lanes(along)]))
    hyper = -jnp.sum(keep * along + move * image) / math.sqrt(n_expert * side.shape[1])
    return (result[None], jnp.reshape(hyper, (1,)))


def solution(mesh):
    finer = Mesh(mesh.devices.reshape(4, 2, 4, 4), EXPERT_FSDP)
    specs = (
        P(EXPERT, None, FSDP),
        P(EXPERT_FSDP, None),
        P(EXPERT_FSDP, None),
        P(EXPERT_FSDP),
        P(),
        P(EXPERT, FSDP, None),
        P(EXPERT, FSDP, None),
    )
    return jax.shard_map(
        local, mesh=finer, in_specs=specs, out_specs=(P(EXPERT, FSDP, None), P()), check_vma=False
    )
```

```python
import math

import jax
import jax.numpy as jnp
from jax import lax
from jax.experimental import pallas as pl
from jax.experimental.pallas import tpu as pltpu
from jax.sharding import Mesh
from jax.sharding import PartitionSpec as P

EXPERT_FSDP = ("expert_0", "expert_1", "fsdp_0", "fsdp_1")
EXPERT = ("expert_0", "expert_1")
FSDP = ("fsdp_0", "fsdp_1")
PARAMS = dict(vmem_limit_bytes=60 * 1024 * 1024)
LANES = 128


def shift(array, axis, amount):
    size = lax.axis_size(axis)
    return lax.ppermute(array, axis, [(i, (i + amount) % size) for i in range(size)])


def pick(array, index):
    return lax.dynamic_index_in_dim(array, index, 0, keepdims=False)


def ring_reduce(blocks, axis):
    own, near, far, back = (blocks[k].astype(jnp.float32) for k in range(4))
    wire = blocks.dtype
    half = far.shape[0] // 2
    far_up = shift(blocks[2, :half], axis, 1).astype(jnp.float32)
    far_down = shift(blocks[2, half:], axis, -1).astype(jnp.float32)
    up = jnp.concatenate([near[:half] + far_up, near[half:]]).astype(wire)
    down = jnp.concatenate([back[:half], back[half:] + far_down]).astype(wire)
    return own + shift(up, axis, 1).astype(jnp.float32) + shift(down, axis, -1).astype(jnp.float32)


def ring_gather(block, axis):
    half = block.shape[0] // 2
    back = shift(block, axis, 1)
    near = shift(block, axis, -1)
    far = [shift(back[:half], axis, 1), shift(near[half:], axis, -1)]
    return jnp.concatenate([block, near] + far + [back]).reshape((4,) + block.shape)


def rolled(array, amount, dim):
    size = array.shape[dim]
    twice = jnp.concatenate([array, array], axis=dim)
    return lax.dynamic_slice_in_dim(twice, amount % size, size, dim)


def gram(hidden):
    row, column = lax.axis_index("fsdp_0"), lax.axis_index("fsdp_1")
    size, depth = hidden.shape
    tiles = hidden.reshape(4, 4, size // 16, depth)
    tiles = rolled(rolled(tiles, column, 0), row, 1)
    partial = lax.dot_general(
        tiles.reshape(size, depth),
        hidden,
        (((1,), (1,)), ((), ())),
        preferred_element_type=jnp.float32,
    ).astype(jnp.bfloat16)
    tiles = ring_reduce(partial.reshape(4, 4, size // 16, size), "fsdp_1")
    block = ring_reduce(tiles.astype(jnp.bfloat16), "fsdp_0").astype(jnp.bfloat16)
    tiles = ring_gather(ring_gather(block, "fsdp_0"), "fsdp_1")
    return rolled(rolled(tiles, -column, 0), -row, 1).reshape(size, size)


def gather_axis(block, axis):
    size = lax.axis_size(axis)
    me = lax.axis_index(axis)
    array = jnp.zeros((size,) + block.shape, block.dtype)
    array = lax.dynamic_update_index_in_dim(array, block, me, 0)
    for step in range(1, size):
        arrived = shift(block, axis, step)
        array = lax.dynamic_update_index_in_dim(array, arrived, (me - step) % size, 0)
    return array


def relative(rows):
    outer, inner = lax.axis_size("expert_0"), lax.axis_size("expert_1")
    chip, core = lax.axis_index("expert_0"), lax.axis_index("expert_1")
    blocks = rows.reshape((outer, inner, -1) + rows.shape[1:])
    blocks = jnp.where(core == 0, blocks, blocks[:, ::-1])
    twice = jnp.concatenate([blocks, blocks], axis=0)
    return lax.dynamic_slice_in_dim(twice, chip, outer, 0).reshape(rows.shape)


def expert_exchange(rows, sign):
    outer, inner = lax.axis_size("expert_0"), lax.axis_size("expert_1")
    block = rows.shape[0] // (outer * inner)
    blocks = rows.reshape((outer, inner, block) + rows.shape[1:])
    other = shift(blocks[:, 1], "expert_1", 1)
    out = []
    for step in range(outer):
        pair = jnp.stack([blocks[step, 0], other[step]])
        out.append(shift(pair, "expert_0", sign * step) if step else pair)
    return jnp.concatenate(out).reshape(rows.shape)


def all_sum(values):
    for axis in EXPERT_FSDP[::-1]:
        size = lax.axis_size(axis)
        values = sum([values] + [shift(values, axis, step) for step in range(1, size)])
    return values


def direct_sum(values):
    size = lax.axis_size(EXPERT_FSDP)
    copies = jnp.broadcast_to(values[None], (size,) + values.shape)
    return jnp.sum(
        lax.all_to_all(copies, EXPERT_FSDP, split_axis=0, concat_axis=0, tiled=True), axis=0
    )


def gate_tables(packed, experts, capacity):
    blocks, tokens, _ = packed.shape
    top = (packed.shape[2] - 1) // 2
    outer, inner = lax.axis_size("expert_0"), lax.axis_size("expert_1")
    chip, core = lax.axis_index("expert_0"), lax.axis_index("expert_1")
    ids = packed[:, :, :top].reshape(blocks, tokens * top).astype(jnp.int32)
    gates = packed[:, :, top : 2 * top].reshape(blocks, tokens * top)
    same = ids[:, :, None] == ids[:, None, :]
    order = jnp.arange(tokens * top)
    earlier = order[None, :] < order[:, None]
    slots = jnp.sum((same & earlier[None]).astype(jnp.int32), axis=2)
    places = (chip - ids // inner) % outer * inner + (core - ids % inner) % inner
    column = places * (blocks * capacity) + jnp.arange(blocks)[:, None] * capacity + slots
    columns = jnp.arange(experts * blocks * capacity)
    hits = column[:, :, None] == columns[None, None, :]
    weighted = jnp.where(hits, gates[:, :, None], 0.0)
    weighted = weighted.reshape(blocks * tokens, top, -1)
    return jnp.sum(weighted, axis=1), packed[:, :, 2 * top].reshape(-1)


def outputs_kernel(place_ref, hidden_ref, side_ref, out_ref, norm_ref, rows_ref):
    width = out_ref.shape[2]
    rows = rows_ref.shape[0]
    block, tile = rows // 8, rows // 3

    @pl.when(pl.program_id(0) == 0)
    def _():
        for k in range(8):
            source = (place_ref[0] + k // 2) % 4 * 2 + (place_ref[1] + k % 2) % 2
            start = pl.multiple_of(source * block, block)
            rows_ref[k * block : (k + 1) * block, :] = hidden_ref[pl.ds(start, block), :]

    @pl.loop(0, 3)
    def _(i):
        part = pl.ds(pl.multiple_of(i * tile, tile), tile)
        product = jnp.dot(rows_ref[part, :], side_ref[...], preferred_element_type=jnp.float32)
        for k in range(2):
            out_ref[k, part, :] = product[:, k * width : (k + 1) * width]

    wide = side_ref[...].astype(jnp.float32)
    square = wide * wide
    norm_ref[0] = jnp.sum(square.reshape(-1, 8, square.shape[1]), axis=0)


def expert_outputs(place, hidden, side):
    rows, depth = hidden.shape
    width = side.shape[1] // 16
    return pl.pallas_call(
        outputs_kernel,
        grid_spec=pltpu.PrefetchScalarGridSpec(
            num_scalar_prefetch=1,
            grid=(8,),
            in_specs=[
                pl.BlockSpec((rows, depth), lambda i, p: (0, 0)),
                pl.BlockSpec((depth, 2 * width), lambda i, p: (0, i)),
            ],
            out_specs=[
                pl.BlockSpec((2, rows, width), lambda i, p: (i, 0, 0)),
                pl.BlockSpec((1, 8, 2 * width), lambda i, p: (i, 0, 0)),
            ],
            scratch_shapes=[pltpu.VMEM((rows, depth), hidden.dtype)],
        ),
        out_shape=[
            jax.ShapeDtypeStruct((16, rows, width), jnp.float32),
            jax.ShapeDtypeStruct((8, 8, 2 * width), jnp.float32),
        ],
        compiler_params=pltpu.CompilerParams(**PARAMS),
        cost_estimate=pl.CostEstimate(
            flops=2 * rows * depth * side.shape[1],
            bytes_accessed=4 * rows * side.shape[1],
            transcendentals=0,
        ),
        name="expert_outputs",
    )(place, hidden, side)


def finish_kernel(
    coef_ref, hidden_ref, tangent_ref, side_ref, target_ref, out_ref, image_ref, along_ref
):
    tangents = jnp.concatenate([tangent_ref[0], tangent_ref[1]], axis=1)
    tile = hidden_ref.shape[0] // 2
    image_ref[...] = jnp.zeros_like(image_ref)
    along_ref[...] = jnp.zeros_like(along_ref)

    @pl.loop(0, 2)
    def _(i):
        part = pl.ds(pl.multiple_of(i * tile, tile), tile)
        image = jnp.dot(hidden_ref[part, :], tangents, preferred_element_type=jnp.float32)
        side = side_ref[part, :].astype(jnp.float32)
        target = target_ref[part, :].astype(jnp.float32)
        out_ref[part, :] = coef_ref[0, 0] * side + coef_ref[1, 0] * image
        image_ref[0] += jnp.sum((target * image).reshape(-1, 8, image.shape[1]), axis=0)
        along_ref[0] += jnp.sum((target * side).reshape(-1, 8, image.shape[1]), axis=0)


def finish(coefs, hidden_t, tangents, side, target):
    width = tangents.shape[2]
    depth, rows = hidden_t.shape
    column = pl.BlockSpec((depth, 2 * width), lambda i: (0, i))
    sums = pl.BlockSpec((1, 8, 2 * width), lambda i: (i, 0, 0))
    sums_shape = jax.ShapeDtypeStruct((8, 8, 2 * width), jnp.float32)
    return pl.pallas_call(
        finish_kernel,
        grid=(8,),
        in_specs=[
            pl.BlockSpec(memory_space=pltpu.SMEM),
            pl.BlockSpec((depth, rows), lambda i: (0, 0)),
            pl.BlockSpec((2, rows, width), lambda i: (i, 0, 0)),
            column,
            column,
        ],
        out_specs=[column, sums, sums],
        out_shape=[jax.ShapeDtypeStruct(side.shape, jnp.float32), sums_shape, sums_shape],
        compiler_params=pltpu.CompilerParams(**PARAMS),
        cost_estimate=pl.CostEstimate(
            flops=2 * rows * depth * side.shape[1],
            bytes_accessed=12 * depth * side.shape[1],
            transcendentals=0,
        ),
        name="finish",
    )(coefs, hidden_t, tangents, side, target)


def mix(table, rows):
    return jnp.dot(
        table, rows, precision=lax.Precision.HIGHEST, preferred_element_type=jnp.float32
    )


def lanes(array):
    return jnp.sum(jnp.sum(array.reshape(-1, array.shape[-1]), axis=0).reshape(-1, LANES), axis=0)


def local(hidden, expert_ids, gate_weights, loss_weight, decay, val_grad, down_weight):
    n_expert = lax.axis_size(EXPERT)
    n_fsdp = lax.axis_size(FSDP)
    capacity = hidden.shape[1] // (n_expert * n_fsdp)
    tokens, top = expert_ids.shape
    rate = decay[0]
    side, target = val_grad[0], down_weight[0]
    place = jnp.stack([lax.axis_index("expert_0"), lax.axis_index("expert_1")]).astype(jnp.int32)
    partial, norm = expert_outputs(place, hidden[0], side)
    rows, width = partial.shape[1:]
    summed = lax.psum_scatter(
        partial.reshape(n_fsdp * rows, width), FSDP, scatter_dimension=0, tiled=True
    )

    packed = jnp.concatenate(
        [expert_ids.astype(jnp.float32), gate_weights, loss_weight[:, None]], axis=1
    )
    packed, stored, norm = lax.optimization_barrier((packed, hidden[0], norm))
    packed = packed.reshape(-1)
    acts = relative(stored)
    share = n_fsdp // n_expert
    for axis in EXPERT_FSDP[::-1]:
        packed = gather_axis(packed, axis)
    everyone = packed.reshape(n_expert, n_fsdp, -1)
    mine = lax.dynamic_slice_in_dim(everyone, lax.axis_index(EXPERT) * share, share, 1)
    mine = mine.swapaxes(0, 1).reshape(share * n_expert, tokens, 2 * top + 1)
    table, weights = gate_tables(mine, n_expert, capacity)
    kernel_matrix = gram(acts)
    acts_t = acts.T
    norm = lanes(norm)
    summed, table, weights, kernel_matrix, acts_t, norm = lax.optimization_barrier(
        (summed, table, weights, kernel_matrix, acts_t, norm)
    )

    mixed = mix(table, expert_exchange(summed, 1))
    scaled = weights[:, None] * mixed
    leaving = mix(table.T, scaled).astype(jnp.bfloat16)
    returned = expert_exchange(leaving, -1)
    gathered = lax.all_gather(returned, FSDP, axis=0, tiled=True)
    tangents = gathered.reshape((n_fsdp,) + returned.shape)

    second = jnp.dot(kernel_matrix, returned, preferred_element_type=jnp.float32)
    again = mix(table, expert_exchange(second.astype(jnp.bfloat16), 1).astype(jnp.float32))
    sums = jnp.stack(
        [
            norm,
            lanes(scaled * mixed),
            lanes(second * returned.astype(jnp.float32)),
            lanes(weights[:, None] * again * again),
        ]
    )
    sums = jnp.sum(all_sum(sums), axis=1, keepdims=True)
    sums = jnp.broadcast_to(sums, (sums.shape[0], LANES))
    bb, bg, gg, ghg = (sums[k] for k in range(4))
    alpha = bb / (bg + rate * bb)
    lean = bg / bb
    across = gg - bg * lean
    fresh = alpha * alpha * across
    beta = fresh / bb
    bent = ghg - 2.0 * lean * gg + lean * lean * bg
    curve = alpha * alpha * (bent + rate * across) - beta * fresh / alpha
    step = fresh / curve
    keep = alpha + step * (beta + alpha * lean)
    move = -step * alpha

    coefs = jnp.stack([keep, move])
    result, image, along = finish(coefs, acts_t, tangents, side, target)
    image, along = direct_sum(jnp.stack([lanes(image), lanes(along)]))
    hyper = -jnp.sum(keep * along + move * image) / math.sqrt(n_expert * side.shape[1])
    return (result[None], jnp.reshape(hyper, (1,)))


def solution(mesh):
    finer = Mesh(mesh.devices.reshape(4, 2, 4, 4), EXPERT_FSDP)
    specs = (
        P(EXPERT, None, FSDP),
        P(EXPERT_FSDP, None),
        P(EXPERT_FSDP, None),
        P(EXPERT_FSDP),
        P(),
        P(EXPERT, FSDP, None),
        P(EXPERT, FSDP, None),
    )
    return jax.shard_map(
        local, mesh=finer, in_specs=specs, out_specs=(P(EXPERT, FSDP, None), P()), check_vma=False
    )
```

```python
import math

import jax
import jax.numpy as jnp
from jax import lax
from jax.experimental import pallas as pl
from jax.experimental.pallas import tpu as pltpu
from jax.sharding import Mesh
from jax.sharding import PartitionSpec as P

EXPERT_FSDP = ("expert_0", "expert_1", "fsdp_0", "fsdp_1")
EXPERT = ("expert_0", "expert_1")
FSDP = ("fsdp_0", "fsdp_1")
PARAMS = dict(vmem_limit_bytes=60 * 1024 * 1024)
LANES = 128


def shift(array, axis, amount):
    size = lax.axis_size(axis)
    return lax.ppermute(array, axis, [(i, (i + amount) % size) for i in range(size)])


def pick(array, index):
    return lax.dynamic_index_in_dim(array, index, 0, keepdims=False)


def ring_reduce(blocks, axis):
    own, near, far, back = (blocks[k].astype(jnp.float32) for k in range(4))
    wire = blocks.dtype
    half = far.shape[0] // 2
    far_up = shift(blocks[2, :half], axis, 1).astype(jnp.float32)
    far_down = shift(blocks[2, half:], axis, -1).astype(jnp.float32)
    up = jnp.concatenate([near[:half] + far_up, near[half:]]).astype(wire)
    down = jnp.concatenate([back[:half], back[half:] + far_down]).astype(wire)
    return own + shift(up, axis, 1).astype(jnp.float32) + shift(down, axis, -1).astype(jnp.float32)


def ring_gather(block, axis):
    half = block.shape[0] // 2
    back = shift(block, axis, 1)
    near = shift(block, axis, -1)
    far = [shift(back[:half], axis, 1), shift(near[half:], axis, -1)]
    return jnp.concatenate([block, near] + far + [back]).reshape((4,) + block.shape)


def rolled(array, amount, dim):
    size = array.shape[dim]
    twice = jnp.concatenate([array, array], axis=dim)
    return lax.dynamic_slice_in_dim(twice, amount % size, size, dim)


def gram(hidden):
    row, column = lax.axis_index("fsdp_0"), lax.axis_index("fsdp_1")
    size, depth = hidden.shape
    tiles = hidden.reshape(4, 4, size // 16, depth)
    tiles = rolled(rolled(tiles, column, 0), row, 1)
    partial = lax.dot_general(
        tiles.reshape(size, depth),
        hidden,
        (((1,), (1,)), ((), ())),
        preferred_element_type=jnp.float32,
    ).astype(jnp.bfloat16)
    tiles = ring_reduce(partial.reshape(4, 4, size // 16, size), "fsdp_1")
    block = ring_reduce(tiles.astype(jnp.bfloat16), "fsdp_0").astype(jnp.bfloat16)
    tiles = ring_gather(ring_gather(block, "fsdp_0"), "fsdp_1")
    return rolled(rolled(tiles, -column, 0), -row, 1).reshape(size, size)


def gather_axis(block, axis):
    size = lax.axis_size(axis)
    me = lax.axis_index(axis)
    array = jnp.zeros((size,) + block.shape, block.dtype)
    array = lax.dynamic_update_index_in_dim(array, block, me, 0)
    for step in range(1, size):
        arrived = shift(block, axis, step)
        array = lax.dynamic_update_index_in_dim(array, arrived, (me - step) % size, 0)
    return array


def relative(rows):
    outer, inner = lax.axis_size("expert_0"), lax.axis_size("expert_1")
    chip, core = lax.axis_index("expert_0"), lax.axis_index("expert_1")
    blocks = rows.reshape((outer, inner, -1) + rows.shape[1:])
    blocks = jnp.where(core == 0, blocks, blocks[:, ::-1])
    twice = jnp.concatenate([blocks, blocks], axis=0)
    return lax.dynamic_slice_in_dim(twice, chip, outer, 0).reshape(rows.shape)


def expert_exchange(rows, sign):
    outer, inner = lax.axis_size("expert_0"), lax.axis_size("expert_1")
    block = rows.shape[0] // (outer * inner)
    blocks = rows.reshape((outer, inner, block) + rows.shape[1:])
    other = shift(blocks[:, 1], "expert_1", 1)
    out = []
    for step in range(outer):
        pair = jnp.stack([blocks[step, 0], other[step]])
        out.append(shift(pair, "expert_0", sign * step) if step else pair)
    return jnp.concatenate(out).reshape(rows.shape)


def all_sum(values):
    for axis in EXPERT_FSDP[::-1]:
        size = lax.axis_size(axis)
        values = sum([values] + [shift(values, axis, step) for step in range(1, size)])
    return values


def direct_sum(values):
    size = lax.axis_size(EXPERT_FSDP)
    copies = jnp.broadcast_to(values[None], (size,) + values.shape)
    return jnp.sum(
        lax.all_to_all(copies, EXPERT_FSDP, split_axis=0, concat_axis=0, tiled=True), axis=0
    )


def gate_tables(packed, experts, capacity):
    blocks, tokens, _ = packed.shape
    top = (packed.shape[2] - 1) // 2
    outer, inner = lax.axis_size("expert_0"), lax.axis_size("expert_1")
    chip, core = lax.axis_index("expert_0"), lax.axis_index("expert_1")
    ids = packed[:, :, :top].reshape(blocks, tokens * top).astype(jnp.int32)
    gates = packed[:, :, top : 2 * top].reshape(blocks, tokens * top)
    same = ids[:, :, None] == ids[:, None, :]
    order = jnp.arange(tokens * top)
    earlier = order[None, :] < order[:, None]
    slots = jnp.sum((same & earlier[None]).astype(jnp.int32), axis=2)
    places = (chip - ids // inner) % outer * inner + (core - ids % inner) % inner
    column = places * (blocks * capacity) + jnp.arange(blocks)[:, None] * capacity + slots
    columns = jnp.arange(experts * blocks * capacity)
    hits = column[:, :, None] == columns[None, None, :]
    weighted = jnp.where(hits, gates[:, :, None], 0.0)
    weighted = weighted.reshape(blocks * tokens, top, -1)
    return jnp.sum(weighted, axis=1), packed[:, :, 2 * top].reshape(-1)


def outputs_kernel(place_ref, hidden_ref, side_ref, out_ref, norm_ref, rows_ref):
    width = out_ref.shape[2]
    block = rows_ref.shape[0] // 8

    @pl.when(pl.program_id(0) == 0)
    def _():
        for k in range(8):
            source = (place_ref[0] + k // 2) % 4 * 2 + (place_ref[1] + k % 2) % 2
            start = pl.multiple_of(source * block, block)
            rows_ref[k * block : (k + 1) * block, :] = hidden_ref[pl.ds(start, block), :]

    product = jnp.dot(rows_ref[...], side_ref[...], preferred_element_type=jnp.float32)
    for k in range(2):
        out_ref[k] = product[:, k * width : (k + 1) * width]

    wide = side_ref[...].astype(jnp.float32)
    square = wide * wide
    norm_ref[0] = jnp.sum(square.reshape(-1, 8, square.shape[1]), axis=0)


def expert_outputs(place, hidden, side):
    rows, depth = hidden.shape
    width = side.shape[1] // 16
    return pl.pallas_call(
        outputs_kernel,
        grid_spec=pltpu.PrefetchScalarGridSpec(
            num_scalar_prefetch=1,
            grid=(8,),
            in_specs=[
                pl.BlockSpec((rows, depth), lambda i, p: (0, 0)),
                pl.BlockSpec((depth, 2 * width), lambda i, p: (0, i)),
            ],
            out_specs=[
                pl.BlockSpec((2, rows, width), lambda i, p: (i, 0, 0)),
                pl.BlockSpec((1, 8, 2 * width), lambda i, p: (i, 0, 0)),
            ],
            scratch_shapes=[pltpu.VMEM((rows, depth), hidden.dtype)],
        ),
        out_shape=[
            jax.ShapeDtypeStruct((16, rows, width), jnp.float32),
            jax.ShapeDtypeStruct((8, 8, 2 * width), jnp.float32),
        ],
        compiler_params=pltpu.CompilerParams(**PARAMS),
        cost_estimate=pl.CostEstimate(
            flops=2 * rows * depth * side.shape[1],
            bytes_accessed=4 * rows * side.shape[1],
            transcendentals=0,
        ),
        name="expert_outputs",
    )(place, hidden, side)


def finish_kernel(coef_ref, hidden_ref, tangent_ref, side_ref, target_ref, out_ref, sums_ref):
    tangents = jnp.concatenate([tangent_ref[0], tangent_ref[1]], axis=1)
    image = jnp.dot(hidden_ref[...], tangents, preferred_element_type=jnp.float32)
    side = side_ref[...].astype(jnp.float32)
    target = target_ref[...].astype(jnp.float32)
    out_ref[...] = coef_ref[0, 0] * side + coef_ref[1, 0] * image

    @pl.when(pl.program_id(0) == 0)
    def _():
        sums_ref[...] = jnp.zeros_like(sums_ref)

    for k, other in enumerate((side, image)):
        sums_ref[k] += jnp.sum((target * other).reshape(-1, 8, image.shape[1]), axis=0)


def finish(coefs, hidden_t, tangents, side, target):
    width = tangents.shape[2]
    depth, rows = hidden_t.shape
    column = pl.BlockSpec((depth, 2 * width), lambda i: (0, i))
    sums = pl.BlockSpec((2, 8, 2 * width), lambda i: (0, 0, 0))
    sums_shape = jax.ShapeDtypeStruct((2, 8, 2 * width), jnp.float32)
    return pl.pallas_call(
        finish_kernel,
        grid=(8,),
        in_specs=[
            pl.BlockSpec(memory_space=pltpu.SMEM),
            pl.BlockSpec((depth, rows), lambda i: (0, 0)),
            pl.BlockSpec((2, rows, width), lambda i: (i, 0, 0)),
            column,
            column,
        ],
        out_specs=[column, sums],
        out_shape=[jax.ShapeDtypeStruct(side.shape, jnp.float32), sums_shape],
        compiler_params=pltpu.CompilerParams(**PARAMS),
        cost_estimate=pl.CostEstimate(
            flops=2 * rows * depth * side.shape[1],
            bytes_accessed=12 * depth * side.shape[1],
            transcendentals=0,
        ),
        name="finish",
    )(coefs, hidden_t, tangents, side, target)


def mix(table, rows):
    return jnp.dot(
        table, rows, precision=lax.Precision.HIGHEST, preferred_element_type=jnp.float32
    )


def lanes(array):
    return jnp.sum(jnp.sum(array.reshape(-1, array.shape[-1]), axis=0).reshape(-1, LANES), axis=0)


def local(hidden, expert_ids, gate_weights, loss_weight, decay, val_grad, down_weight):
    n_expert = lax.axis_size(EXPERT)
    n_fsdp = lax.axis_size(FSDP)
    capacity = hidden.shape[1] // (n_expert * n_fsdp)
    tokens, top = expert_ids.shape
    rate = decay[0]
    side, target = val_grad[0], down_weight[0]
    place = jnp.stack([lax.axis_index("expert_0"), lax.axis_index("expert_1")]).astype(jnp.int32)
    partial, norm = expert_outputs(place, hidden[0], side)
    rows, width = partial.shape[1:]
    summed = lax.psum_scatter(
        partial.reshape(n_fsdp * rows, width), FSDP, scatter_dimension=0, tiled=True
    )

    packed = jnp.concatenate(
        [expert_ids.astype(jnp.float32), gate_weights, loss_weight[:, None]], axis=1
    )
    packed, stored, norm = lax.optimization_barrier((packed, hidden[0], norm))
    packed = packed.reshape(-1)
    acts = relative(stored)
    share = n_fsdp // n_expert
    for axis in EXPERT_FSDP[::-1]:
        packed = gather_axis(packed, axis)
    everyone = packed.reshape(n_expert, n_fsdp, -1)
    mine = lax.dynamic_slice_in_dim(everyone, lax.axis_index(EXPERT) * share, share, 1)
    mine = mine.swapaxes(0, 1).reshape(share * n_expert, tokens, 2 * top + 1)
    table, weights = gate_tables(mine, n_expert, capacity)
    kernel_matrix = gram(acts)
    acts_t = acts.T
    norm = lanes(norm)
    summed, table, weights, kernel_matrix, acts_t, norm = lax.optimization_barrier(
        (summed, table, weights, kernel_matrix, acts_t, norm)
    )

    mixed = mix(table, expert_exchange(summed, 1))
    scaled = weights[:, None] * mixed
    leaving = mix(table.T, scaled).astype(jnp.bfloat16)
    returned = expert_exchange(leaving, -1)
    gathered = lax.all_gather(returned, FSDP, axis=0, tiled=True)
    tangents = gathered.reshape((n_fsdp,) + returned.shape)

    second = jnp.dot(kernel_matrix, returned, preferred_element_type=jnp.float32)
    again = mix(table, expert_exchange(second.astype(jnp.bfloat16), 1).astype(jnp.float32))
    sums = jnp.stack(
        [
            norm,
            lanes(scaled * mixed),
            lanes(second * returned.astype(jnp.float32)),
            lanes(weights[:, None] * again * again),
        ]
    )
    sums = jnp.sum(all_sum(sums), axis=1, keepdims=True)
    sums = jnp.broadcast_to(sums, (sums.shape[0], LANES))
    bb, bg, gg, ghg = (sums[k] for k in range(4))
    alpha = bb / (bg + rate * bb)
    lean = bg / bb
    across = gg - bg * lean
    fresh = alpha * alpha * across
    beta = fresh / bb
    bent = ghg - 2.0 * lean * gg + lean * lean * bg
    curve = alpha * alpha * (bent + rate * across) - beta * fresh / alpha
    step = fresh / curve
    keep = alpha + step * (beta + alpha * lean)
    move = -step * alpha

    coefs = jnp.stack([keep, move])
    result, sums = finish(coefs, acts_t, tangents, side, target)
    along, image = direct_sum(jnp.sum(sums.reshape(2, -1, LANES), axis=1))
    hyper = -jnp.sum(keep * along + move * image) / math.sqrt(n_expert * side.shape[1])
    return (result[None], jnp.reshape(hyper, (1,)))


def solution(mesh):
    finer = Mesh(mesh.devices.reshape(4, 2, 4, 4), EXPERT_FSDP)
    specs = (
        P(EXPERT, None, FSDP),
        P(EXPERT_FSDP, None),
        P(EXPERT_FSDP, None),
        P(EXPERT_FSDP),
        P(),
        P(EXPERT, FSDP, None),
        P(EXPERT, FSDP, None),
    )
    return jax.shard_map(
        local, mesh=finer, in_specs=specs, out_specs=(P(EXPERT, FSDP, None), P()), check_vma=False
    )
```
